32 devices in a mesh: parts: 2 (over y), gz: 8 (over z, x), gy: 2 (over core).
Axes of the slice: x: 2, y: 2, z: 4, core: 2. Of those that a mesh axis runs over, the one named last changes fastest.
Arguments:
- direction: float32 [3, 16, 128, 128], P(None, ('parts', 'gz'), 'gy'), parts along dimension 1, may hold values from -6 to 6
- region: int32 [16, 128, 128], P(('parts', 'gz'), 'gy'), parts along dimension 0, may hold values from 0 to 3
- saturation: float32 [3], replicated, may hold values from 0.5 to 2
- kernel_main: float32 [6, 16, 256, 128], P(None, 'gz', 'gy'), may hold values from -6 to 6
- kernel_nyq: float32 [6, 16, 256], P(None, 'gz', 'gy'), may hold values from -6 to 6
Outputs:
- field: float32 [3, 16, 128, 128], P(None, ('parts', 'gz'), 'gy'), parts along dimension 1
The draws below stay inside these ranges and needn't reach their ends.
There are 2 independent parts, one for each index of `parts`. The reference program is written for one: setup_inputs(seed, part) draws one part's arguments, and reference() takes and returns one part's arrays. A program takes and returns all parts, laid end to end along the dimension named above; an argument that names none is the same for every part. Nothing has to cross between parts.
Inputs may be any that keep to these rules, and one draw needn't show every extreme that they name: `region`: 0 marks an empty cell; other ids name materials.
All inputs are finite; a program needn't handle non-finite values.
Results may differ from the reference program's by a relative error of at most 0.00007.
Values sent between devices are 32-bit elements; how exact they have to be, the bound alone decides.
A program may use at most 64 MiB of HBM per device.

```python
import math
import jax
import jax.numpy as jnp
import numpy as np

MX = 128
MY = 128
REGIONS = 4
MZ = 8
PY = 256
PZ = 16
ZBITS = 3


def touch_ends(array, key, smallest, largest):
    place = [jax.random.randint(jax.random.fold_in(key, axis), (), 0, length) for axis, length in enumerate(array.shape)]
    longest = array.shape.index(max(array.shape))
    neighbour = place[:longest] + [(place[longest] + 1) % array.shape[longest]] + place[longest + 1:]
    return array.at[tuple(place)].set(smallest).at[tuple(neighbour)].set(largest)


def level_of(own_key, dims, cuts, least, high):
    loudness, own = 1.0, jax.random.fold_in(own_key, 6)
    for dim, shards_of in cuts:
        draws = jnp.exp(jax.random.uniform(jax.random.fold_in(own, dim), (shards_of,), jnp.float32, least / len(cuts), high / len(cuts)))
        loudness = loudness * jnp.repeat(draws, dims[dim] // shards_of).reshape([-1 if axis == dim else 1 for axis in range(len(dims))])
    return loudness


def noise(rng, extent, deviation, reach, cuts=(), dtype=jnp.bfloat16):
    entries = jax.random.normal(rng, extent, jnp.float32) * deviation
    if len(cuts) > 0:
        entries = level_of(rng, extent, cuts, -0.22, 0.18) * entries
    return jnp.clip(entries, min=-reach, max=reach).astype(dtype)


def setup_inputs(seed: int = 0, part: int = 0) -> dict:
    seeds = jax.random.split(jax.random.key(seed), 6)
    part_keys = jax.random.split(jax.random.fold_in(seeds[5], part), 6)
    return {
        "direction": noise(part_keys[0], (3, MZ, MY, MX), 1.0, 6.0, ((1, 8), (2, 2)), jnp.float32),
        "region": touch_ends(jax.random.randint(part_keys[1], (MZ, MY, MX), 0, REGIONS), jax.random.fold_in(part_keys[1], 1), 0, REGIONS - 1).astype(jnp.int32),
        "saturation": jnp.clip(jnp.exp(jax.random.uniform(seeds[2], (REGIONS - 1,), jnp.float32, math.log(0.5), math.log(2.0))), 0.5, 2.0),
        "kernel_main": noise(seeds[3], (6, PZ, PY, MX), 1.0, 6.0, ((1, 8), (2, 2)), jnp.float32),
        "kernel_nyq": noise(seeds[4], (6, PZ, PY), 1.0, 6.0, ((1, 8), (2, 2)), jnp.float32),
    }


exchange_stiffness = 0.25
tensor_index = ((0, 3, 4), (3, 1, 5), (4, 5, 2))


def slot_order(bit_count):
    slot_index = np.arange(2 ** (bit_count + 1))
    device = slot_index // 2
    reversed_bits = device * 0
    for b in range(bit_count):
        reversed_bits = reversed_bits + ((device >> b) & 1) * (2 ** (bit_count - 1 - b))
    return 2 * reversed_bits + slot_index % 2


def neighbours(padded):
    summed = padded[..., 2:, 1:-1, 1:-1] + padded[..., :-2, 1:-1, 1:-1]
    summed = summed + padded[..., 1:-1, 2:, 1:-1] + padded[..., 1:-1, :-2, 1:-1]
    return summed + padded[..., 1:-1, 1:-1, 2:] + padded[..., 1:-1, 1:-1, :-2]


def reference(direction, region, saturation, kernel_main, kernel_nyq):
    magnetic = (region > 0).astype(jnp.float32)
    strength = jnp.zeros(region.shape, jnp.float32)
    for r in range(REGIONS - 1):
        strength = strength + jnp.where(region == r + 1, saturation[r], 0.0)
    moment = direction * strength[None]
    padded = jnp.zeros((3, 2 * MZ, 2 * MY, 2 * MX), jnp.float32).at[:, :MZ, :MY, :MX].set(moment)
    spectra = jnp.fft.rfftn(padded, axes=(1, 2, 3))
    inverse_slots = np.argsort(slot_order(ZBITS)).astype(np.int32)
    kernel = jnp.concatenate([kernel_main, kernel_nyq[..., None]], axis=3)[:, inverse_slots]
    pieces = []
    for i in range(3):
        summed = kernel[tensor_index[i][0]] * spectra[0]
        for j in (1, 2):
            summed = summed + kernel[tensor_index[i][j]] * spectra[j]
        pieces.append(summed)
    demag = jnp.fft.irfftn(jnp.stack(pieces), s=(2 * MZ, 2 * MY, 2 * MX), axes=(1, 2, 3))
    demag = demag[:, :MZ, :MY, :MX]
    moment_rim = jnp.pad(direction * magnetic[None], ((0, 0), (1, 1), (1, 1), (1, 1)))
    count_rim = jnp.pad(magnetic, 1)
    near = neighbours(moment_rim)
    count = neighbours(count_rim)
    exchange = exchange_stiffness * magnetic[None] * (near - count[None] * direction)
    return (demag + exchange).astype(jnp.float32)
```

```python
import functools
import math

import jax
import jax.numpy as jnp
import numpy as np
from jax import lax
from jax.experimental import pallas as pl
from jax.experimental.pallas import tpu as pltpu
from jax.sharding import PartitionSpec as P

exchange_stiffness = 0.25
tensor_index = ((0, 3, 4), (3, 1, 5), (4, 5, 2))
highest = lax.Precision.HIGHEST


def with_halo(cells, sides, width):
    for axis, dim in sides:
        count = lax.axis_size(axis)
        ends = count - 1
        head = lax.slice_in_dim(cells, 0, width, axis=dim)
        tail = lax.slice_in_dim(cells, cells.shape[dim] - width, cells.shape[dim], axis=dim)
        cells = jnp.concatenate(
            [
                lax.ppermute(tail, axis, [(i, (i + 1) % count) for i in range(ends)]),
                cells,
                lax.ppermute(head, axis, [((i + 1) % count, i) for i in range(ends)]),
            ],
            axis=dim,
        )
    return cells


def phase(first, second, period):
    product = first[:, None] * second[None, :] % period
    angle = 2.0 * math.pi / period * product.astype(jnp.float32)
    return (jnp.cos(angle), jnp.sin(angle))


def slot_frequency(slot_index, bit_count):
    device = slot_index // 2
    reversed_bits = jnp.zeros_like(device)
    for b in range(bit_count):
        reversed_bits = reversed_bits + device // 2**b % 2 * 2 ** (bit_count - 1 - b)
    return 2 * reversed_bits + slot_index % 2


def row_transform(plane):
    columns = plane.shape[2]
    row_count = plane.shape[1]
    positions = jnp.arange(columns, dtype=jnp.int32)
    cosine, sine = phase(positions, positions, 2 * columns)
    table = jnp.concatenate([cosine, -sine], axis=1)
    flat = plane.reshape(3 * row_count, columns)
    both = jnp.dot(flat, table, precision=highest).reshape(3, row_count, 2, columns)
    signs = 1.0 - 2.0 * (positions % 2).astype(jnp.float32)
    nyquist = jnp.dot(flat, signs, precision=highest).reshape(3, row_count)
    return (both[:, :, 0], both[:, :, 1], nyquist)


def column_transform(real_rows, imag_rows, nyquist, cosine, sine):
    new_real = jnp.einsum("kr,crx->ckx", cosine, real_rows, precision=highest) + jnp.einsum(
        "kr,crx->ckx", sine, imag_rows, precision=highest
    )
    new_imag = jnp.einsum("kr,crx->ckx", cosine, imag_rows, precision=highest) - jnp.einsum(
        "kr,crx->ckx", sine, real_rows, precision=highest
    )
    nyq_real = jnp.einsum("kr,cr->ck", cosine, nyquist, precision=highest)
    nyq_imag = -jnp.einsum("kr,cr->ck", sine, nyquist, precision=highest)
    return (jnp.stack([new_real, new_imag], axis=1), jnp.stack([nyq_real, nyq_imag], axis=1))


def plane_transform(values, cosine, sine, direction_sign):
    real_part = values[:, 0]
    imag_part = values[:, 1]
    new_real = jnp.einsum(
        "pz,cz...->cp...", cosine, real_part, precision=highest
    ) - direction_sign * jnp.einsum("pz,cz...->cp...", sine, imag_part, precision=highest)
    new_imag = jnp.einsum(
        "pz,cz...->cp...", cosine, imag_part, precision=highest
    ) + direction_sign * jnp.einsum("pz,cz...->cp...", sine, real_part, precision=highest)
    return jnp.stack([new_real, new_imag], axis=1)


def apply_kernel(spectra, kernel):
    pieces = []
    for i in range(3):
        summed = kernel[tensor_index[i][0]] * spectra[0]
        for j in (1, 2):
            summed = summed + kernel[tensor_index[i][j]] * spectra[j]
        pieces.append(summed)
    return jnp.stack(pieces)


def local(direction, region, saturation, kernel_main, kernel_nyq):
    columns = direction.shape[3]
    own_rows = direction.shape[2]
    groups_y = lax.axis_size("gy")
    groups_z = lax.axis_size("gz")
    bit_count = groups_z.bit_length() - 1
    rows_total = own_rows * groups_y
    period_y = 2 * rows_total
    period_z = 2 * groups_z
    period_x = 2 * columns
    spec_rows = period_y // groups_y
    y_index = lax.axis_index("gy")
    magnetic = (region > 0).astype(jnp.float32)
    strength = jnp.zeros(region.shape, jnp.float32)
    for r in range(saturation.shape[0]):
        strength = strength + jnp.where(region == r + 1, saturation[r], 0.0)
    magnet_plane = (direction * strength[None])[:, 0]
    gathered = lax.all_gather(magnet_plane, "gy", axis=1, tiled=True)
    frequency = y_index * spec_rows + jnp.arange(spec_rows, dtype=jnp.int32)
    cosine, sine = phase(frequency, jnp.arange(rows_total, dtype=jnp.int32), period_y)
    real_rows, imag_rows, nyquist = row_transform(gathered)
    spec_main, spec_nyq = column_transform(real_rows, imag_rows, nyquist, cosine, sine)
    slot_freq = slot_frequency(jnp.arange(period_z, dtype=jnp.int32), bit_count)
    plane_ids = jnp.arange(groups_z, dtype=jnp.int32)
    sent_main, sent_nyq = (
        lax.all_to_all(spec_main[:, :, None], "gz", split_axis=3, concat_axis=2, tiled=True),
        lax.all_to_all(spec_nyq[:, :, None], "gz", split_axis=3, concat_axis=2, tiled=True),
    )
    cosine, sine = phase(slot_freq, plane_ids, period_z)
    done_main = plane_transform(sent_main, cosine, sine, -1.0)
    done_nyq = plane_transform(sent_nyq, cosine, sine, -1.0)
    full_main, full_nyq = (
        lax.all_to_all(done_main, "gz", split_axis=2, concat_axis=3, tiled=True),
        lax.all_to_all(done_nyq, "gz", split_axis=2, concat_axis=3, tiled=True),
    )
    field_main = apply_kernel(full_main, kernel_main)
    field_nyq = apply_kernel(full_nyq, kernel_nyq)
    out_main, out_nyq = (
        lax.all_to_all(field_main, "gz", split_axis=3, concat_axis=2, tiled=True),
        lax.all_to_all(field_nyq, "gz", split_axis=3, concat_axis=2, tiled=True),
    )
    cosine, sine = phase(plane_ids, slot_freq, period_z)
    back_main = plane_transform(out_main, cosine, sine, 1.0)
    back_nyq = plane_transform(out_nyq, cosine, sine, 1.0)
    plane_main, plane_nyq = (
        lax.all_to_all(back_main, "gz", split_axis=2, concat_axis=3, tiled=True),
        lax.all_to_all(back_nyq, "gz", split_axis=2, concat_axis=3, tiled=True),
    )
    plane_main = plane_main[:, :, 0]
    plane_nyq = plane_nyq[:, :, 0]
    frequency = y_index * spec_rows + jnp.arange(spec_rows, dtype=jnp.int32)
    cosine, sine = phase(jnp.arange(rows_total, dtype=jnp.int32), frequency, period_y)
    term_real = jnp.einsum("yk,ckx->cyx", cosine, plane_main[:, 0], precision=highest) - jnp.einsum(
        "yk,ckx->cyx", sine, plane_main[:, 1], precision=highest
    )
    term_imag = jnp.einsum("yk,ckx->cyx", cosine, plane_main[:, 1], precision=highest) + jnp.einsum(
        "yk,ckx->cyx", sine, plane_main[:, 0], precision=highest
    )
    nyq_real = jnp.einsum("yk,ck->cy", cosine, plane_nyq[:, 0], precision=highest) - jnp.einsum(
        "yk,ck->cy", sine, plane_nyq[:, 1], precision=highest
    )
    nyq_imag = jnp.einsum("yk,ck->cy", cosine, plane_nyq[:, 1], precision=highest) + jnp.einsum(
        "yk,ck->cy", sine, plane_nyq[:, 0], precision=highest
    )
    rows_main, rows_nyq = (
        lax.psum_scatter(
            jnp.stack([term_real, term_imag], axis=1), "gy", scatter_dimension=2, tiled=True
        ),
        lax.psum_scatter(
            jnp.stack([nyq_real, nyq_imag], axis=1), "gy", scatter_dimension=2, tiled=True
        ),
    )
    positions = jnp.arange(columns, dtype=jnp.int32)
    cosine, sine = phase(positions, positions, period_x)
    weights = jnp.where(positions == 0, 1.0, 2.0).astype(jnp.float32)[:, None]
    table = jnp.concatenate([weights * cosine, -weights * sine], axis=0)
    flat = jnp.concatenate([rows_main[:, 0], rows_main[:, 1]], axis=2).reshape(
        3 * own_rows, 2 * columns
    )
    signs = 1.0 - 2.0 * (positions % 2).astype(jnp.float32)
    demag = jnp.dot(flat, table, precision=highest).reshape(3, own_rows, columns)
    demag = demag + rows_nyq[:, 0][:, :, None] * signs[None, None, :]
    demag = demag * (1.0 / (period_x * period_y * period_z))
    moment = direction * magnetic[None]
    stacked = jnp.concatenate([moment, magnetic[None]], axis=0)
    rim = with_halo(stacked, (("gz", 1), ("gy", 2)), 1)
    centre = rim[:, 1:2, 1:-1]
    near = rim[:, 0:1, 1:-1] + rim[:, 2:3, 1:-1] + rim[:, 1:2, :-2] + rim[:, 1:2, 2:]
    padded_x = jnp.pad(centre, ((0, 0), (0, 0), (0, 0), (1, 1)))
    near = near + padded_x[..., :-2] + padded_x[..., 2:]
    exchange = exchange_stiffness * magnetic[None] * (near[:3] - near[3:4] * direction)
    return demag[:, None] + exchange


MESH = pl.DeviceIdType.MESH
line_chips = 4
scope = jax.named_scope


def halves(table):
    high = table.astype(np.float32).astype(jnp.bfloat16)
    low = (table - high.astype(np.float64)).astype(np.float32).astype(jnp.bfloat16)
    return np.stack([high, low])


@functools.lru_cache(maxsize=None)
def tables(columns, rows_total, groups_z):
    x = np.arange(columns)
    ang = np.pi / columns * (np.outer(x, x) % (2 * columns))
    c, s = np.cos(ang), np.sin(ang)
    fwd = np.block([[c, -s], [s, c]])
    w = np.where(x == 0, 1.0, 2.0)[:, None]
    inv = np.block([[w * c, w * s], [-w * s, w * c]])
    tx = np.stack([halves(fwd), halves(inv)])
    ky = np.arange(2 * rows_total)
    ang = np.pi / rows_total * (np.outer(ky, np.arange(rows_total)) % (2 * rows_total))
    c, s = np.cos(ang), np.sin(ang)
    f = np.block([[c, s], [-s, c]])
    scale = 1.0 / (4 * rows_total * columns * 2 * groups_z)
    pick = np.zeros((2, 3, 12, columns))
    for slot in range(2):
        for d in range(3):
            for i in range(3):
                pick[slot, d, tensor_index[i][(i + d) % 3] * 2 + slot, i] = 1.0
    bits = groups_z.bit_length() - 1
    coef = np.zeros((groups_z, 2, 1, max(columns, 4 * groups_z)))
    plane = np.arange(groups_z)
    for g in range(groups_z):
        rev = sum(((g >> b) & 1) << (bits - 1 - b) for b in range(bits))
        for core in range(2):
            for k in range(2):
                slot = (core + k) % 2
                ang = np.pi / groups_z * ((2 * rev + slot) * plane % (2 * groups_z))
                coef[g, core, 0, 2 * k : 4 * groups_z : 4] = np.cos(ang)
                coef[g, core, 0, 2 * k + 1 : 4 * groups_z : 4] = -np.sin(ang)
    return (
        tx,
        halves(f),
        halves(f.T * scale),
        pick.astype(np.float32),
        coef.astype(np.float32),
    )


def split(value):
    high = value.astype(jnp.bfloat16)
    return high, (value - high.astype(jnp.float32)).astype(jnp.bfloat16)


def mm(a, b):
    return jnp.dot(a, b, preferred_element_type=jnp.float32)


def mm3(a, b):
    return mm(a[0], b[0]) + mm(a[1], b[0]) + mm(a[0], b[1])


def when(cond, action):
    pl.when(cond)(action)


def fused(
    coef_hbm,
    sat_hbm,
    direction_hbm,
    region_hbm,
    pick_hbm,
    knyq_hbm,
    kmain_hbm,
    tx_hbm,
    tyf_hbm,
    tyi_hbm,
    out,
    coef,
    sat,
    direction,
    region,
    pick,
    knyq,
    nfac,
    mom,
    strength,
    near_strength,
    edge_out,
    edge_in,
    kfull,
    tx,
    tyf,
    tyi,
    zh,
    zl,
    xs,
    xr,
    nown,
    rh,
    rl,
    spectra,
    part,
    gh,
    gl,
    nback,
    afull,
    apeer,
    xsend,
    xrecv,
    zsend,
    zmid,
    zin,
    load_sem,
    side_ssem,
    side_rsem,
    zown_ssem,
    relay_ssem,
    z_rsem,
    s_ssem,
    s_rsem,
    e_ssem,
    e_rsem,
    k_ssem,
    k_rsem,
    xs_ssem,
    xs_rsem,
    a_ssem,
    a_rsem,
    rx_ssem,
    rx_rsem,
    rz_ssem,
    rm_rsem,
    rz_rsem,
):
    line = mom.shape[1]
    planes = 2 * line
    rows = mom.shape[3]
    columns = mom.shape[4]
    rows_total = 2 * rows
    spec = kmain_hbm.shape[2]
    freqs = 2 * spec
    g = lax.axis_index("gz")
    c = lax.axis_index("gy")
    o = g // 2
    xi = g % 2
    own = pl.ds(pl.multiple_of(c * rows, rows), rows)
    other = pl.ds(pl.multiple_of((1 - c) * rows, rows), rows)
    own_im = pl.ds(pl.multiple_of(rows_total + c * rows, rows), rows)
    other_im = pl.ds(pl.multiple_of(rows_total + (1 - c) * rows, rows), rows)
    own_freqs = pl.ds(pl.multiple_of(c * spec, spec), spec)
    peer_id = {"gz": g, "gy": 1 - c}
    side_id = {"gz": g + 1 - 2 * xi, "gy": c}

    def chip(steps):
        return {"gz": g + 2 * steps, "gy": c}

    has = {k: (o + k < line) if k > 0 else (o + k >= 0) for k in (1, -1, 2, -2, 3, -3)}
    after_id = {"gz": g + 1, "gy": c}
    before_id = {"gz": g - 1, "gy": c}
    has_after = g < planes - 1
    has_before = g > 0
    inner = jnp.logical_and(o > 0, o < line - 1)
    lower = o < line // 2

    barrier = pltpu.get_barrier_semaphore()
    friends = 2
    for where in (peer_id, side_id):
        pl.semaphore_signal(barrier, inc=1, device_id=where, device_id_type=MESH)
    for cond, where in [(has[k], chip(k)) for k in (1, -1, 2, -2)] + [(has_after, after_id), (has_before, before_id)]:
        friends = friends + jnp.where(cond, 1, 0)

        @pl.when(cond)
        def _(where=where):
            pl.semaphore_signal(barrier, inc=1, device_id=where, device_id_type=MESH)

    first = [
        pltpu.make_async_copy(region_hbm, region, load_sem.at[0]),
        pltpu.make_async_copy(sat_hbm, sat, load_sem.at[1]),
        pltpu.make_async_copy(direction_hbm, direction, load_sem.at[2]),
    ]
    for copy in first:
        copy.start()
    loads = [
        pltpu.make_async_copy(coef_hbm.at[g, c], coef, load_sem.at[3]),
        pltpu.make_async_copy(tx_hbm, tx, load_sem.at[4]),
        pltpu.make_async_copy(tyf_hbm, tyf, load_sem.at[5]),
        pltpu.make_async_copy(tyi_hbm, tyi, load_sem.at[6]),
        pltpu.make_async_copy(pick_hbm.at[c], pick, load_sem.at[7]),
        pltpu.make_async_copy(knyq_hbm, knyq.at[c], load_sem.at[8]),
        pltpu.make_async_copy(kmain_hbm.at[:, c], kfull.at[:, own_freqs, :], load_sem.at[9]),
    ]
    with scope("s01_load"):
        for copy in first:
            copy.wait()
    for copy in loads:
        copy.start()

    reg = region[0]
    s = jnp.zeros(reg.shape, jnp.float32)
    for r in range(sat_hbm.shape[0]):
        s = s + jnp.where(reg == r + 1, sat[r], 0.0)
    strength[...] = s
    for j in range(3):
        mom[xi, o, j] = direction[j, 0] * s
    brim = pl.ds(pl.multiple_of((1 - c) * (rows - 8), 8), 8)
    there = jnp.where(region[0, brim, :] > 0, 1.0, 0.0)
    for j in range(3):
        edge_out[j] = direction[j, 0, brim, :] * there
    edge_out[3] = there

    with scope("s02_barrier"):
        pl.semaphore_wait(barrier, friends)

    def remote(src, dst, ssem, rsem, where):
        return pltpu.make_async_remote_copy(
            src_ref=src, dst_ref=dst, send_sem=ssem, recv_sem=rsem, device_id=where, device_id_type=MESH
        )

    def z_copy(d, j, ssem, steps):
        block = mom.at[xi, d, j]
        return remote(block, block, ssem, z_rsem.at[d, j], chip(steps))

    def side_copy(d, j):
        block = mom.at[xi, d, j]
        return remote(block, block, side_ssem.at[0], side_rsem.at[j], side_id)

    ways = (1, -1, 2, -2)
    with scope("s03_send"):
        for j in range(3):
            for w, k in enumerate(ways):
                when(has[k], lambda: z_copy(o, j, zown_ssem.at[w], k).start())
            side_copy(o, j).start()
        edge = remote(edge_out, edge_in, e_ssem.at[0], e_rsem.at[0], peer_id)
        edge.start()
        swap_main = remote(
            kmain_hbm.at[:, 1 - c], kfull.at[:, own_freqs, :], k_ssem.at[0], k_rsem.at[0], peer_id
        )
        swap_main.start()
        swap_nyq = remote(knyq_hbm, knyq.at[c], k_ssem.at[1], k_rsem.at[1], peer_id)
        swap_nyq.start()

    def passing(k, j):
        d = o + k

        @pl.when(has[k])
        def _():
            z_copy(d, j, zown_ssem.at[0], -k).wait_recv()
            if k == 2:
                when(has[-1], lambda: z_copy(d, j, relay_ssem.at[1], -1).start())
            if k == -2:
                when(has[1], lambda: z_copy(d, j, relay_ssem.at[0], 1).start())
            side_copy(d, j).start()

    with scope("s04_ag"):
        for j in range(3):
            for k in (-1, 1, -2, 2):
                passing(k, j)
    with scope("s05_ag3"):
        for j in range(3):
            for k in (-3, 3):
                passing(k, j)

    def strength_copy(way):
        return remote(
            strength, near_strength.at[way], s_ssem.at[way], s_rsem.at[way], (after_id, before_id)[way]
        )

    when(has_after, lambda: strength_copy(0).start())
    when(has_before, lambda: strength_copy(1).start())
    with scope("s06_loads"):
        for copy in loads:
            copy.wait()
        swap_main.wait_recv()
        swap_nyq.wait_recv()

    lane = lax.broadcasted_iota(jnp.int32, (rows, columns), 1)
    signs = 1.0 - 2.0 * (lane % 2).astype(jnp.float32)
    signs_total = jnp.concatenate([signs, signs], axis=0)
    for h in range(2):
        factors = knyq[h].reshape(12, spec)
        for d in range(3):
            nfac[d, h * spec : (h + 1) * spec, :] = lax.dot_general(
                factors, pick[d], (((0,), (0,)), ((), ())), precision=highest, preferred_element_type=jnp.float32
            )

    def swap_copy(j):
        return remote(xs.at[j], xr.at[j], xs_ssem.at[0], xs_rsem.at[j], peer_id)

    def store_rows(target, re, im, block):
        lanes = slice(block * columns, (block + 1) * columns)
        for at, value in zip(target, (re, im), strict=True):
            hi, lo = split(value)
            rh[at, lanes] = hi
            rl[at, lanes] = lo

    step = 32
    for j in range(3):
        with scope("s07_wait%d" % j):
            remote(
                mom.at[1 - xi, :, j], mom.at[1 - xi, :, j], side_ssem.at[0], side_rsem.at[j], side_id
            ).wait_recv()
        with scope("s08_zx%d" % j):
            place = jnp.logical_or(lane[:step] == j, lane[:step] == j + 3)
            for top in range(0, rows, step):
                band = slice(top, top + step)
                accs = [None] * 4
                for p in range(planes):
                    m = mom[p % 2, p // 2, j, band, :]
                    for q in range(4):
                        term = m * coef[0, 4 * p + q]
                        accs[q] = term if accs[q] is None else accs[q] + term
                for q in range(4):
                    hi, lo = split(accs[q])
                    at = (q // 2) * rows + top
                    lanes = slice((q % 2) * columns, (q % 2 + 1) * columns)
                    zh[at : at + step, lanes] = hi
                    zl[at : at + step, lanes] = lo
                    total = jnp.sum(accs[q] * signs[:step], axis=1, keepdims=True)
                    if q < 2:
                        nown[q, band, :] = jnp.where(place, total, nown[q, band, :] if j > 0 else 0.0)
                    else:
                        xs[3, q - 2, band, :] = jnp.where(place, total, xs[3, q - 2, band, :] if j > 0 else 0.0)
            res = mm3((zh[...], zl[...]), (tx[0, 0], tx[0, 1]))
            for q in range(2):
                xs[j, q] = res[rows:, q * columns : (q + 1) * columns]
            swap_copy(j).start()
            if j == 2:
                swap_copy(3).start()
            store_rows((own, own_im), res[:rows, :columns], res[:rows, columns:], j)

    wide = 2 * columns

    def forward(pair):
        lanes = slice(pair * wide, (pair + 1) * wide)
        spectra[pair] = mm3((tyf[0], tyf[1]), (rh[:, lanes], rl[:, lanes]))

    def take(j):
        swap_copy(j).wait_recv()
        store_rows((other, other_im), xr[j, 0], xr[j, 1], j)

    blocks = [slice(b, b + 64) for b in range(0, freqs, 64)]
    with scope("s09_take01"):
        store_rows((own, own_im), nown[0], nown[1], 3)
        take(0)
        take(1)
    with scope("s10_y01"):
        forward(0)
        for i in range(3):
            for block in blocks:
                k0 = kfull[tensor_index[i][0], block, :]
                k1 = kfull[tensor_index[i][1], block, :]
                for q in range(2):
                    at = slice(q * freqs + block.start, q * freqs + block.stop)
                    part[i, at, :] = k0 * spectra[0, at, :columns] + k1 * spectra[0, at, columns:]
    with scope("s11_take23"):
        take(2)
        take(3)
    with scope("s12_y23"):
        forward(1)

    homes = (0, 2, 3)

    def multiply(i):
        lanes = slice(homes[i] * columns, (homes[i] + 1) * columns)
        for block in blocks:
            k2 = kfull[tensor_index[i][2], block, :]
            for q in range(2):
                at = slice(q * freqs + block.start, q * freqs + block.stop)
                hi, lo = split(part[i, at, :] + k2 * spectra[1, at, :columns])
                gh[at, lanes] = hi
                gl[at, lanes] = lo

    def backward(pair):
        lanes = slice(pair * wide, (pair + 1) * wide)
        return mm3((tyi[0], tyi[1]), (gh[:, lanes], gl[:, lanes]))

    def a_copy(j):
        return remote(afull.at[j, :, other, :], apeer.at[j], a_ssem.at[0], a_rsem.at[j], peer_id)

    def finish(i, re, im):
        re, im = split(re), split(im)
        both = [jnp.concatenate([re[h], im[h]], axis=1) for h in range(2)]
        res = mm3(both, (tx[1, 0], tx[1, 1]))
        for q in range(2):
            nyquist = nback[q * rows_total : (q + 1) * rows_total, i : i + 1]
            afull[i, q] = res[:, q * columns : (q + 1) * columns] + nyquist * signs_total
        a_copy(i).start()

    with scope("s13_apply0"):
        multiply(0)
        for q in range(2):
            at = slice(q * freqs, (q + 1) * freqs)
            spectrum = spectra[1, at, columns:]
            total = nfac[0] * spectrum
            for d in (1, 2):
                total = total + nfac[d] * pltpu.roll(spectrum, columns - d, 1)
            hi, lo = split(total)
            gh[at, columns:wide] = hi
            gl[at, columns:wide] = lo
    with scope("s14_inv0"):
        back = backward(0)
        nback[...] = back[:, columns:]
        finish(0, back[:rows_total, :columns], back[rows_total:, :columns])
    with scope("s15_inv12"):
        multiply(1)
        multiply(2)
        back = backward(1)
        for i in (1, 2):
            lanes = slice((i - 1) * columns, i * columns)
            finish(i, back[:rows_total, lanes], back[rows_total:, lanes])

    def contribution(p, j):
        total = None
        for q in range(4):
            a = afull[j, q, own, :] if q < 2 else apeer[j, q - 2]
            term = a * coef[0, 4 * p + q]
            total = term if total is None else total + term
        return total

    last = line - 1
    targets = [
        jnp.where(lower, last, 0),
        jnp.where(o == 0, 2, jnp.where(o == 1, 0, jnp.where(o == 2, last, 1))),
        jnp.where(o == 0, 1, jnp.where(o == last, 2, jnp.where(o == 1, 2, 1))),
        o,
    ]

    def rx_copy(d, j):
        return remote(xsend.at[d, j], xrecv.at[d, j], rx_ssem.at[0], rx_rsem.at[d, j], side_id)

    def side_send(d, j):
        xsend[d, j] = contribution(2 * d + 1 - xi, j)
        rx_copy(d, j).start()

    for j in range(3):
        with scope("s16_a%d" % j):
            a_copy(j).wait_recv()
        with scope("s17_xs%d" % j):
            side_send(targets[0], j)
    with scope("s18_xs"):
        for d in targets[1:]:
            for j in range(3):
                side_send(d, j)

    def exchange():
        edge.wait_recv()
        for way, cond in ((0, has_before), (1, has_after)):

            @pl.when(cond)
            def _(way=way):
                strength_copy(way).wait_recv()

            @pl.when(jnp.logical_not(cond))
            def _(way=way):
                near_strength[way] = jnp.zeros(near_strength.shape[1:], jnp.float32)

        present = jnp.where(region[0] > 0, 1.0, 0.0)
        row_id = lax.broadcasted_iota(jnp.int32, present.shape, 0)
        col_id = lax.broadcasted_iota(jnp.int32, present.shape, 1)

        def plane_near(v, j):
            above = jnp.where(c == 1, edge_in[j, 7:8, :], 0.0)
            below = jnp.where(c == 0, edge_in[j, 0:1, :], 0.0)
            total = jnp.where(row_id > 0, pltpu.roll(v, 1, 0), above)
            total = total + jnp.where(row_id < rows - 1, pltpu.roll(v, rows - 1, 0), below)
            total = total + jnp.where(col_id > 0, pltpu.roll(v, 1, 1), 0.0)
            return total + jnp.where(col_id < columns - 1, pltpu.roll(v, columns - 1, 1), 0.0)

        adjacent = []
        for way in range(2):
            near_s = near_strength[way]
            filled = near_s > 0
            adjacent.append(
                (jnp.where(filled, 1.0 / jnp.where(filled, near_s, 1.0), 0.0), jnp.where(filled, 1.0, 0.0))
            )
        count = plane_near(present, 3) + adjacent[0][1] + adjacent[1][1]
        mask = exchange_stiffness * present
        before = jnp.maximum(g - 1, 0)
        after = jnp.minimum(g + 1, planes - 1)
        for j in range(3):
            near = plane_near(direction[j, 0] * present, j)
            near = near + mom[before % 2, before // 2, j] * adjacent[0][0]
            near = near + mom[after % 2, after // 2, j] * adjacent[1][0]
            out[j, 0] = mask * (near - count * direction[j, 0])

    with scope("s19_exch"):
        exchange()

    def to_target(r, j, kind, steps):
        return remote(zsend.at[r, j], zin.at[kind, j], rz_ssem.at[0], rz_rsem.at[kind, j], chip(steps))

    def to_middle(j, steps):
        return remote(zsend.at[0, j], zmid.at[j], rz_ssem.at[0], rm_rsem.at[j], chip(steps))

    def merge(r, j):
        d = targets[r]
        rx_copy(d, j).wait_recv()
        zsend[r, j] = contribution(2 * d + xi, j) + xrecv[d, j]

    with scope("s20_far"):
        for j in range(3):
            merge(0, j)
            when(o == 0, lambda: to_middle(j, 1).start())
            when(o == last, lambda: to_middle(j, -1).start())
    with scope("s21_r1"):
        for j in range(3):
            merge(1, j)
            when(o == 0, lambda: to_target(1, j, 2, 2).start())
            when(o == last, lambda: to_target(1, j, 2, -2).start())
            when(o == 1, lambda: to_target(1, j, 1, -1).start())
            when(o == 2, lambda: to_target(1, j, 0, 1).start())
    with scope("s22_mid"):
        for j in range(3):

            @pl.when(inner)
            def _():
                to_middle(j, 1).wait_recv()
                zsend[0, j] = zsend[0, j] + zmid[j]
                when(o == 1, lambda: to_target(0, j, 2, 2).start())
                when(o == 2, lambda: to_target(0, j, 2, -2).start())

    with scope("s23_r2"):
        for j in range(3):
            merge(2, j)
            when(lower, lambda: to_target(2, j, 0, 1).start())
            when(jnp.logical_not(lower), lambda: to_target(2, j, 1, -1).start())
    with scope("s24_final"):
        for j in range(3):
            rx_copy(o, j).wait_recv()
            out[j, 0] = out[j, 0] + contribution(g, j) + xrecv[o, j]
        for j in range(3):
            for kind, cond in ((0, has[-1]), (1, has[1]), (2, None)):

                def add():
                    to_target(0, j, kind, 1).wait_recv()
                    out[j, 0] = out[j, 0] + zin[kind, j]

                if cond is None:
                    add()
                else:
                    when(cond, add)

    with scope("s25_drain"):
        remote(mom.at[xi], mom.at[xi], side_ssem.at[0], side_rsem.at[0], side_id).wait_send()
        three = mom.at[xi, 0]
        for w, k in enumerate(ways):
            when(has[k], lambda: remote(three, three, zown_ssem.at[w], z_rsem.at[0, 0], peer_id).wait_send())
        for w, cond in ((0, o == line - 2), (1, o == 1)):
            when(cond, lambda: remote(three, three, relay_ssem.at[w], z_rsem.at[0, 0], peer_id).wait_send())
        when(has_after, lambda: strength_copy(0).wait_send())
        when(has_before, lambda: strength_copy(1).wait_send())
        edge.wait_send()
        swap_main.wait_send()
        swap_nyq.wait_send()
        remote(xs, xr, xs_ssem.at[0], xs_rsem.at[0], peer_id).wait_send()
        remote(afull.at[:, :, other, :], apeer, a_ssem.at[0], a_rsem.at[0], peer_id).wait_send()
        remote(xsend, xrecv, rx_ssem.at[0], rx_rsem.at[0, 0], side_id).wait_send()
        remote(zsend, zin, rz_ssem.at[0], rz_rsem.at[0, 0], peer_id).wait_send()


def fused_local(direction, region, saturation, kernel_main, kernel_nyq):
    rows, columns = direction.shape[2:]
    planes = lax.axis_size("gz")
    rows_total = 2 * rows
    spec = kernel_main.shape[2]
    freqs = 2 * spec
    line = planes // 2
    tx, tyf, tyi, pick, coef = (jnp.asarray(t) for t in tables(columns, rows_total, planes))
    f32, bf16 = jnp.float32, jnp.bfloat16
    hbm = pl.BlockSpec(memory_space=pltpu.HBM)
    dma = pltpu.SemaphoreType.DMA

    def vmem(*shape, dtype=f32):
        return pltpu.VMEM(shape, dtype)

    operands = (coef, saturation, direction, region, pick, kernel_nyq, kernel_main, tx, tyf, tyi)
    return pl.pallas_call(
        fused,
        out_shape=pltpu.VMEM(direction.shape, f32),
        in_specs=[hbm] * len(operands),
        out_specs=pl.BlockSpec(memory_space=pltpu.VMEM),
        scratch_shapes=[
            pltpu.SMEM(coef.shape[2:], f32),
            pltpu.SMEM(saturation.shape, f32),
            vmem(*direction.shape),
            vmem(*region.shape, dtype=jnp.int32),
            vmem(*pick.shape[1:]),
            vmem(2, *kernel_nyq.shape),
            vmem(3, freqs, columns),
            vmem(2, line, 3, rows, columns),
            vmem(rows, columns),
            vmem(2, rows, columns),
            vmem(4, 8, columns),
            vmem(4, 8, columns),
            vmem(6, freqs, columns),
            vmem(*tx.shape, dtype=bf16),
            vmem(*tyf.shape, dtype=bf16),
            vmem(*tyi.shape, dtype=bf16),
            vmem(2 * rows, 2 * columns, dtype=bf16),
            vmem(2 * rows, 2 * columns, dtype=bf16),
            vmem(4, 2, rows, columns),
            vmem(4, 2, rows, columns),
            vmem(2, rows, columns),
            vmem(2 * rows_total, 4 * columns, dtype=bf16),
            vmem(2 * rows_total, 4 * columns, dtype=bf16),
            vmem(2, 2 * freqs, 2 * columns),
            vmem(3, 2 * freqs, columns),
            vmem(2 * freqs, 4 * columns, dtype=bf16),
            vmem(2 * freqs, 4 * columns, dtype=bf16),
            vmem(2 * rows_total, columns),
            vmem(3, 2, rows_total, columns),
            vmem(3, 2, rows, columns),
            vmem(line, 3, rows, columns),
            vmem(line, 3, rows, columns),
            vmem(3, 3, rows, columns),
            vmem(3, rows, columns),
            vmem(3, 3, rows, columns),
            dma((10,)),
            dma((1,)),
            dma((3,)),
            dma((4,)),
            dma((2,)),
            dma((line, 3)),
            dma((2,)),
            dma((2,)),
            dma((1,)),
            dma((1,)),
            dma((2,)),
            dma((2,)),
            dma((1,)),
            dma((4,)),
            dma((1,)),
            dma((3,)),
            dma((1,)),
            dma((line, 3)),
            dma((1,)),
            dma((3,)),
            dma((3, 3)),
        ],
        compiler_params=pltpu.CompilerParams(
            collective_id=0, has_side_effects=True, vmem_limit_bytes=32 * 1024 * 1024
        ),
        name="field_kernel",
    )(*(pltpu.with_memory_space_constraint(t, pltpu.HBM) for t in operands))


def solution(mesh):
    placed = (
        P(None, ("parts", "gz"), "gy", None),
        P(("parts", "gz"), "gy", None),
        P(),
        P(None, "gz", "gy", None),
        P(None, "gz", "gy"),
    )
    small = mesh.shape["gz"] == 2 * line_chips and mesh.shape["gy"] == 2
    return jax.shard_map(
        fused_local if small else local,
        mesh=mesh,
        in_specs=placed,
        out_specs=P(None, ("parts", "gz"), "gy", None),
        check_vma=False,
    )
```
